32 devices in a mesh: grp: 8 (over y, x, core), wide: 4 (over z).
Axes of the slice: x: 2, y: 2, z: 4, core: 2. Of those that a mesh axis runs over, the one named last changes fastest.
Arguments:
- gradient: bfloat16 [8, 4, 16, 4096], P('grp', 'wide'), may hold values from -6 to 6
- residual: float32 [8, 4, 16, 4096], P('grp', 'wide'), may hold values from -4 to 4
- selected: int32 [8, 4, 4, 32], P('grp', 'wide'), may hold values from 0 to 127, as said below
- counts: int32 [8, 4, 4], P('grp', 'wide'), may hold values from 1 to 32, as said below
Outputs:
- update: float32 [4, 4, 4096], P('wide')
- new_residual: float32 [8, 4, 16, 4096], P('grp', 'wide')
The draws below stay inside these ranges and needn't reach their ends.
Inputs may be any that keep to these rules, and one draw needn't show every extreme that they name: `selected`: for each device and shard, 32 distinct block numbers of that shard; entries at or past the count are ignored. `counts`: one shard has 32 on every device; every device has at most one other shard at 32, the rest at most 16.
All inputs are finite; a program needn't handle non-finite values.
Results may differ from the reference program's by a relative error of at most 0.0003.
Values sent between devices are 32-bit elements; how exact they have to be, the bound alone decides.
No kernel may reach another device: no remote copies, remote signals or barrier semaphores. Data moves between devices by JAX's collectives and lax.ppermute only.
A program may use at most 64 MiB of HBM per device.

```python
import jax
import jax.numpy as jnp

D = 4096
BW = 128
OWN_ROWS = 4
W_ROWS = 16
OWN_BLK = 128
KMAX = 32
N_GRP = 8
N_WIDE = 4


def draw_selected(key, part):
    scores = jax.random.randint(key, (N_GRP, N_WIDE, N_WIDE, OWN_BLK), 0, 1 << 20)
    scores = scores * OWN_BLK + jnp.arange(OWN_BLK, dtype=jnp.int32)
    order = jnp.argsort(scores, axis=-1)
    return order[..., :KMAX].astype(jnp.int32)


def draw_counts(key, part):
    first, second, third = jax.random.split(jax.random.fold_in(key, 7), 3)
    base = jax.random.randint(first, (N_GRP, N_WIDE, N_WIDE), max(1, KMAX // 8), KMAX // 2 + 1)
    common = jax.random.randint(second, (), 0, N_WIDE)
    personal = jax.random.randint(third, (N_GRP, N_WIDE, 1), 0, N_WIDE)
    shard = jnp.arange(N_WIDE, dtype=jnp.int32)[None, None, :]
    hottest = jnp.logical_or(shard == common, shard == personal)
    return jnp.where(hottest, KMAX, base).astype(jnp.int32)


def levels(key, dims, cuts, least, high):
    level, own = 1.0, jax.random.fold_in(key, 6)
    for dim, shards_of in cuts:
        steps = jnp.exp(jax.random.uniform(jax.random.fold_in(own, dim), (shards_of,), jnp.float32, least / len(cuts), high / len(cuts)))
        level = level * jnp.repeat(steps, dims[dim] // shards_of).reshape([-1 if axis == dim else 1 for axis in range(len(dims))])
    return level


def gaussian(rng, extent, deviation, limit, pieces=(), held_as=jnp.bfloat16):
    factor_of = levels(rng, extent, pieces, -0.22, 0.18) if pieces else 1.0
    result = jax.random.normal(rng, extent, jnp.float32) * deviation * factor_of
    return jnp.minimum(jnp.maximum(result, -limit), limit).astype(held_as)


def setup_inputs(seed: int = 0) -> dict:
    seeds = jax.random.split(jax.random.key(seed), 5)
    return {
        "gradient": gaussian(seeds[0], (N_GRP, N_WIDE, W_ROWS, D), 1.0, 6.0, ((0, 8), (1, 4))),
        "residual": gaussian(seeds[1], (N_GRP, N_WIDE, W_ROWS, D), 0.5, 4.0, ((0, 8), (1, 4)), jnp.float32),
        "selected": draw_selected(jax.random.fold_in(seeds[4], 71), 0),
        "counts": draw_counts(jax.random.fold_in(seeds[4], 71), 0),
    }


def reference(gradient, residual, selected, counts):
    accumulated = gradient.astype(jnp.float32) + residual
    blocks = accumulated.reshape(N_GRP, N_WIDE, N_WIDE, OWN_BLK, BW)
    slot_ids = jnp.arange(KMAX, dtype=jnp.int32)
    valid = (slot_ids[None, None, None, :] < counts[..., None]).astype(jnp.float32)
    block_ids = jnp.arange(OWN_BLK, dtype=jnp.int32)
    hits = (selected[..., None] == block_ids).astype(jnp.float32)
    mask = jnp.sum(hits * valid[..., None], axis=3)
    new_residual = (blocks * (1.0 - mask[..., None])).reshape(N_GRP, N_WIDE, W_ROWS, D)
    total = jnp.sum(blocks * mask[..., None], axis=(0, 1))
    update = (total / N_GRP).reshape(N_WIDE, OWN_ROWS, D)
    return update, new_residual
```

```python
import jax
import jax.numpy as jnp
from jax import lax
from jax.experimental import pallas as pl
from jax.experimental.pallas import tpu as pltpu
from jax.sharding import PartitionSpec as P

LANES = 128
PAD = 8


def is_pow2(n):
    return n & (n - 1) == 0


def fill_blocks(grad, res, acc):
    for c in range(acc.shape[0]):
        at = pl.ds(c * LANES, LANES)
        acc[c] = grad[:, at].astype(jnp.float32) + res[:, at]


def pick_call(grad, res, sel, cnt, info, shards, own_rows, by_xor):
    rows, width = grad.shape
    cols = width // LANES
    slots = sel.shape[1]
    per = LANES // slots

    def kernel(info_s, cnt_s, sel_s, sel_v, grad_v, res_v, *rest):
        outs, acc = rest[:-1], rest[-1]
        fill_blocks(grad_v, res_v, acc)
        me = info_s[0]
        lane = lax.broadcasted_iota(jnp.int32, (1, LANES), 1)

        def pack(shard, off, put):
            for k in range(slots):
                b = sel_s[shard, k]
                row = shard * own_rows + b // cols
                put(k, 1, acc[b % cols, pl.ds(row, 1), :])
            ids = sel_v[pl.ds(shard, 1), :]
            ids = (ids % cols) * own_rows + ids // cols
            ids = jnp.concatenate([ids] * per, axis=1)
            keep = (lane // slots == off) & (lane % slots < cnt_s[shard])
            ids = jnp.where(keep, ids, -1).astype(jnp.float32)
            put(slots, PAD, jnp.broadcast_to(ids, (PAD, LANES)))

        if by_xor:
            for j in range(shards):

                def put(at, n, value, out=outs[j]):
                    out[at : at + n, :] = value

                pack(me ^ j, j % per, put)
        else:
            def step(j, carry):
                def put(at, n, value):
                    outs[0][j, at : at + n, :] = value

                pack(j, me % per, put)
                return carry

            lax.fori_loop(0, shards, step, 0)

    smem = pl.BlockSpec(memory_space=pltpu.SMEM)
    vmem = pl.BlockSpec(memory_space=pltpu.VMEM)
    size = (slots + PAD, LANES)
    shapes = [jax.ShapeDtypeStruct(size, jnp.float32)] * shards
    if not by_xor:
        shapes = [jax.ShapeDtypeStruct((shards,) + size, jnp.float32)]
    return pl.pallas_call(
        kernel,
        out_shape=shapes,
        in_specs=[smem, smem, smem, vmem, vmem, vmem],
        out_specs=[vmem] * len(shapes),
        scratch_shapes=[pltpu.VMEM((cols, rows, LANES), jnp.float32)],
        name="pick",
    )(info, cnt, sel, sel, grad, res)


def keep_call(grad, res, sel, cnt, own_rows):
    rows, width = grad.shape
    cols = width // LANES
    shards, slots = sel.shape

    def kernel(cnt_s, sel_s, grad_v, res_v, out, acc):
        fill_blocks(grad_v, res_v, acc)
        zero = jnp.zeros((1, LANES), jnp.float32)

        def step(s, carry):
            used = cnt_s[s]
            for k in range(slots):
                b = sel_s[s, k]

                @pl.when(k < used)
                def _():
                    acc[b % cols, pl.ds(s * own_rows + b // cols, 1), :] = zero

            return carry

        lax.fori_loop(0, shards, step, 0)
        for c in range(cols):
            out[:, c * LANES : (c + 1) * LANES] = acc[c]

    smem = pl.BlockSpec(memory_space=pltpu.SMEM)
    vmem = pl.BlockSpec(memory_space=pltpu.VMEM)
    return pl.pallas_call(
        kernel,
        out_shape=jax.ShapeDtypeStruct((rows, width), jnp.float32),
        in_specs=[smem, smem, vmem, vmem],
        out_specs=vmem,
        scratch_shapes=[pltpu.VMEM((cols, rows, LANES), jnp.float32)],
        cost_estimate=pl.CostEstimate(flops=10**7, bytes_accessed=10**6, transcendentals=0),
        name="keep",
    )(cnt, sel, grad, res)


def merge_call(parts, slots, own_blocks):
    per = LANES // slots

    def kernel(*refs):
        out = refs[-1]
        views = []
        for ref in refs[:-1]:
            views += [ref] if len(ref.shape) == 2 else [ref.at[i] for i in range(ref.shape[0])]
        block = lax.broadcasted_iota(jnp.int32, (own_blocks, LANES), 0).astype(jnp.float32)
        total = jnp.zeros((own_blocks, LANES), jnp.float32)
        for at in range(0, len(views), per):
            group = views[at : at + per]
            ids = group[0][slots : slots + 1, :]
            for view in group[1:]:
                ids = jnp.maximum(ids, view[slots : slots + 1, :])
            x = [view[:slots, :] for view in group]
            x += [jnp.zeros((slots, LANES), jnp.float32)] * (per - len(group))
            x = jnp.concatenate(x, axis=0)
            hot = (block == ids).astype(jnp.float32).astype(jnp.bfloat16)
            high = x.astype(jnp.bfloat16)
            left = x - high.astype(jnp.float32)
            mid = left.astype(jnp.bfloat16)
            low = (left - mid.astype(jnp.float32)).astype(jnp.bfloat16)
            for piece in (high, mid, low):
                total = total + jnp.dot(hot, piece, preferred_element_type=jnp.float32)
        out[...] = total

    vmem = pl.BlockSpec(memory_space=pltpu.VMEM)
    return pl.pallas_call(
        kernel,
        out_shape=jax.ShapeDtypeStruct((own_blocks, LANES), jnp.float32),
        in_specs=[vmem] * len(parts),
        out_specs=vmem,
        name="merge",
    )(*parts)


def xor_send(x, axis, size, k):
    return lax.ppermute(x, axis, [(i, i ^ k) for i in range(size)])


def group_sum(x, groups):
    if not is_pow2(groups):
        return jnp.sum(lax.all_gather(x, "grp"), axis=0)
    bit = 1
    while bit < groups:
        wide = bit > 1 and bit * 2 < groups
        hops = (bit, 2 * bit, 3 * bit) if wide else (bit,)
        x = sum([xor_send(x, "grp", groups, k) for k in hops], x)
        bit *= 4 if wide else 2
    return x


def make_body(groups, shards):
    by_xor = is_pow2(shards) and shards <= 8

    def body(gradient, residual, selected, counts):
        rows, width = gradient.shape[2:]
        own_rows = rows // shards
        own_blocks = own_rows * width // LANES
        slots = selected.shape[3]
        grad, res, sel, cnt = gradient[0, 0], residual[0, 0], selected[0, 0], counts[0, 0]
        info = lax.axis_index("wide").astype(jnp.int32).reshape(1)
        packed = pick_call(grad, res, sel, cnt, info, shards, own_rows, by_xor)
        if by_xor:
            parts = [packed[0]] + [xor_send(packed[k], "wide", shards, k) for k in range(1, shards)]
        else:
            parts = [lax.all_to_all(packed[0], "wide", split_axis=0, concat_axis=0, tiled=True)]
        new_residual = keep_call(grad, res, sel, cnt, own_rows)[None, None]
        partial = merge_call(parts, slots, own_blocks)
        total = group_sum(partial, groups) / groups
        update = total.reshape(width // LANES, own_rows, LANES).transpose(1, 0, 2)
        return (update.reshape(1, own_rows, width), new_residual)

    return body


def solution(mesh):
    return jax.shard_map(
        make_body(mesh.shape["grp"], mesh.shape["wide"]),
        mesh=mesh,
        in_specs=(
            P("grp", "wide", None, None),
            P("grp", "wide", None, None),
            P("grp", "wide", None, None),
            P("grp", "wide", None),
        ),
        out_specs=(P("wide", None, None), P("grp", "wide", None, None)),
        check_vma=False,
    )
```

```python
import jax
import jax.numpy as jnp
from jax import lax
from jax.experimental import pallas as pl
from jax.experimental.pallas import tpu as pltpu
from jax.sharding import PartitionSpec as P

LANES = 128
PAD = 8


def is_pow2(n):
    return n & (n - 1) == 0


def fill_blocks(grad, res, acc):
    for c in range(acc.shape[0]):
        at = pl.ds(c * LANES, LANES)
        acc[c] = grad[:, at].astype(jnp.float32) + res[:, at]


def pick_call(grad, res, sel, cnt, info, shards, own_rows, by_xor):
    rows, width = grad.shape
    cols = width // LANES
    slots = sel.shape[1]
    per = LANES // slots

    def kernel(info_s, cnt_s, sel_s, sel_v, grad_v, res_v, *rest):
        outs, acc = rest[:-1], rest[-1]
        fill_blocks(grad_v, res_v, acc)
        me = info_s[0]
        lane = lax.broadcasted_iota(jnp.int32, (1, LANES), 1)

        def pack(shard, off, put):
            for k in range(slots):
                b = sel_s[shard, k]
                row = shard * own_rows + b // cols
                put(k, 1, acc[b % cols, pl.ds(row, 1), :])
            ids = sel_v[pl.ds(shard, 1), :]
            ids = (ids % cols) * own_rows + ids // cols
            ids = jnp.concatenate([ids] * per, axis=1)
            keep = (lane // slots == off) & (lane % slots < cnt_s[shard])
            ids = jnp.where(keep, ids, -1).astype(jnp.float32)
            put(slots, PAD, jnp.broadcast_to(ids, (PAD, LANES)))

        if by_xor:
            for j in range(shards):

                def put(at, n, value, out=outs[j]):
                    out[at : at + n, :] = value

                pack(me ^ j, j % per, put)
        else:
            def step(j, carry):
                def put(at, n, value):
                    outs[0][j, at : at + n, :] = value

                pack(j, me % per, put)
                return carry

            lax.fori_loop(0, shards, step, 0)

    smem = pl.BlockSpec(memory_space=pltpu.SMEM)
    vmem = pl.BlockSpec(memory_space=pltpu.VMEM)
    size = (slots + PAD, LANES)
    shapes = [pltpu.VMEM(size, jnp.float32)] * shards
    if not by_xor:
        shapes = [jax.ShapeDtypeStruct((shards,) + size, jnp.float32)]
    return pl.pallas_call(
        kernel,
        out_shape=shapes,
        in_specs=[smem, smem, smem, vmem, vmem, vmem],
        out_specs=[vmem] * len(shapes),
        scratch_shapes=[pltpu.VMEM((cols, rows, LANES), jnp.float32)],
        name="pick",
    )(info, cnt, sel, sel, grad, res)


def keep_call(grad, res, sel, cnt, own_rows):
    rows, width = grad.shape
    cols = width // LANES
    shards, slots = sel.shape

    def kernel(cnt_s, sel_s, grad_v, res_v, out, acc):
        fill_blocks(grad_v, res_v, acc)
        zero = jnp.zeros((1, LANES), jnp.float32)

        def step(s, carry):
            used = cnt_s[s]
            for k in range(slots):
                b = sel_s[s, k]

                @pl.when(k < used)
                def _():
                    acc[b % cols, pl.ds(s * own_rows + b // cols, 1), :] = zero

            return carry

        lax.fori_loop(0, shards, step, 0)
        for c in range(cols):
            out[:, c * LANES : (c + 1) * LANES] = acc[c]

    smem = pl.BlockSpec(memory_space=pltpu.SMEM)
    vmem = pl.BlockSpec(memory_space=pltpu.VMEM)
    return pl.pallas_call(
        kernel,
        out_shape=jax.ShapeDtypeStruct((rows, width), jnp.float32),
        in_specs=[smem, smem, vmem, vmem],
        out_specs=vmem,
        scratch_shapes=[pltpu.VMEM((cols, rows, LANES), jnp.float32)],
        cost_estimate=pl.CostEstimate(flops=10**7, bytes_accessed=10**6, transcendentals=0),
        name="keep",
    )(cnt, sel, grad, res)


def merge_call(parts, slots, own_blocks, chunk):
    per = LANES // slots

    def kernel(*refs):
        out = refs[-1]
        views = []
        for ref in refs[:-1]:
            views += [ref] if len(ref.shape) == 2 else [ref.at[i] for i in range(ref.shape[0])]
        block = lax.broadcasted_iota(jnp.int32, (own_blocks, LANES), 0).astype(jnp.float32)
        total = jnp.zeros((own_blocks, LANES), jnp.float32)
        for at in range(0, len(views), chunk):
            group = views[at : at + chunk]
            ids = group[0][slots : slots + 1, :]
            for view in group[1:]:
                ids = jnp.maximum(ids, view[slots : slots + 1, :])
            x = [view[:slots, :] for view in group]
            x += [jnp.zeros((slots, LANES), jnp.float32)] * (per - len(group))
            x = jnp.concatenate(x, axis=0)
            hot = (block == ids).astype(jnp.float32).astype(jnp.bfloat16)
            high = x.astype(jnp.bfloat16)
            left = x - high.astype(jnp.float32)
            mid = left.astype(jnp.bfloat16)
            low = (left - mid.astype(jnp.float32)).astype(jnp.bfloat16)
            for piece in (high, mid, low):
                total = total + jnp.dot(hot, piece, preferred_element_type=jnp.float32)
        out[...] = total

    vmem = pl.BlockSpec(memory_space=pltpu.VMEM)
    return pl.pallas_call(
        kernel,
        out_shape=pltpu.VMEM((own_blocks, LANES), jnp.float32),
        in_specs=[vmem] * len(parts),
        out_specs=vmem,
        name="merge",
    )(*[pltpu.with_memory_space_constraint(p, pltpu.VMEM) for p in parts])


def xor_send(x, axis, size, k):
    return lax.ppermute(x, axis, [(i, i ^ k) for i in range(size)])


def group_sum(x, groups, bit):
    if not is_pow2(groups):
        return jnp.sum(lax.all_gather(x, "grp"), axis=0)
    while bit < groups:
        wide = bit > 1 and bit * 2 < groups
        hops = (bit, 2 * bit, 3 * bit) if wide else (bit,)
        x = sum([xor_send(x, "grp", groups, k) for k in hops], x)
        bit *= 4 if wide else 2
    return x


def make_body(groups, shards):
    by_xor = is_pow2(shards) and shards <= 8
    early = by_xor and is_pow2(groups) and groups > 1

    def body(gradient, residual, selected, counts):
        rows, width = gradient.shape[2:]
        own_rows = rows // shards
        own_blocks = own_rows * width // LANES
        slots = selected.shape[3]
        grad, res, sel, cnt = gradient[0, 0], residual[0, 0], selected[0, 0], counts[0, 0]
        info = lax.axis_index("wide").astype(jnp.int32).reshape(1)
        packed = pick_call(grad, res, sel, cnt, info, shards, own_rows, by_xor)
        if by_xor:
            parts = [xor_send(packed[k], "wide", shards, k) for k in reversed(range(1, shards))]
            parts = [packed[0]] + parts[::-1]
            if early:
                parts += [xor_send(part, "grp", groups, 1) for part in parts]
        else:
            parts = [lax.all_to_all(packed[0], "wide", split_axis=0, concat_axis=0, tiled=True)]
        new_residual = keep_call(grad, res, sel, cnt, own_rows)[None, None]
        chunk = min(LANES // slots, shards)
        partial = merge_call(parts, slots, own_blocks, chunk)
        total = group_sum(partial, groups, 2 if early else 1) / groups
        update = total.reshape(width // LANES, own_rows, LANES).transpose(1, 0, 2)
        return (update.reshape(1, own_rows, width), new_residual)

    return body


def solution(mesh):
    return jax.shard_map(
        make_body(mesh.shape["grp"], mesh.shape["wide"]),
        mesh=mesh,
        in_specs=(
            P("grp", "wide", None, None),
            P("grp", "wide", None, None),
            P("grp", "wide", None, None),
            P("grp", "wide", None),
        ),
        out_specs=(P("wide", None, None), P("grp", "wide", None, None)),
        check_vma=False,
    )
```

```python
import jax
import jax.numpy as jnp
from jax import lax
from jax.experimental import pallas as pl
from jax.experimental.pallas import tpu as pltpu
from jax.sharding import PartitionSpec as P


LANES = 128
PAD = 8


def is_pow2(n):
    return n & (n - 1) == 0


def row_and_col(b, cols):
    if is_pow2(cols):
        return b >> (cols.bit_length() - 1), b & (cols - 1)
    return b // cols, b % cols


def fill_blocks(grad, res, acc):
    for c in range(acc.shape[0]):
        at = pl.ds(c * LANES, LANES)
        acc[c] = grad[:, at].astype(jnp.float32) + res[:, at]


def pick_call(grad, res, sel, cnt, info, shards, own_rows, by_xor):
    rows, width = grad.shape
    cols = width // LANES
    slots = sel.shape[1]
    per = LANES // slots

    def kernel(info_s, cnt_s, sel_s, sel_v, grad_v, res_v, *rest):
        outs, acc = rest[:-1], rest[-1]
        fill_blocks(grad_v, res_v, acc)
        me = info_s[0]
        lane = lax.broadcasted_iota(jnp.int32, (1, LANES), 1)

        def pack(shard, off, put):
            for k in range(slots):
                row, col = row_and_col(sel_s[shard, k], cols)
                put(k, 1, acc[col, pl.ds(shard * own_rows + row, 1), :])
            ids = sel_v[pl.ds(shard, 1), :]
            row, col = row_and_col(ids, cols)
            ids = col * own_rows + row
            ids = jnp.concatenate([ids] * per, axis=1)
            keep = (lane // slots == off) & (lane % slots < cnt_s[shard])
            ids = jnp.where(keep, ids, -1).astype(jnp.float32)
            put(slots, PAD, jnp.broadcast_to(ids, (PAD, LANES)))

        if by_xor:
            for j in range(shards):

                def put(at, n, value, out=outs[j]):
                    out[at : at + n, :] = value

                pack(me ^ j, j % per, put)
        else:
            def step(j, carry):
                def put(at, n, value):
                    outs[0][j, at : at + n, :] = value

                pack(j, me % per, put)
                return carry

            lax.fori_loop(0, shards, step, 0)

    smem = pl.BlockSpec(memory_space=pltpu.SMEM)
    vmem = pl.BlockSpec(memory_space=pltpu.VMEM)
    size = (slots + PAD, LANES)
    shapes = [pltpu.VMEM(size, jnp.float32)] * shards
    if not by_xor:
        shapes = [jax.ShapeDtypeStruct((shards,) + size, jnp.float32)]
    return pl.pallas_call(
        kernel,
        out_shape=shapes,
        in_specs=[smem, smem, smem, vmem, vmem, vmem],
        out_specs=[vmem] * len(shapes),
        scratch_shapes=[pltpu.VMEM((cols, rows, LANES), jnp.float32)],
        name="pick",
    )(info, cnt, sel, sel, grad, res)


def keep_call(grad, res, sel, cnt, own_rows):
    rows, width = grad.shape
    cols = width // LANES
    shards, slots = sel.shape

    def kernel(cnt_s, sel_s, grad_v, res_v, out, acc):
        fill_blocks(grad_v, res_v, acc)
        zero = jnp.zeros((1, LANES), jnp.float32)

        def step(s, carry):
            used = cnt_s[s]
            for k in range(slots):
                row, col = row_and_col(sel_s[s, k], cols)

                @pl.when(k < used)
                def _():
                    acc[col, pl.ds(s * own_rows + row, 1), :] = zero

            return carry

        lax.fori_loop(0, shards, step, 0)
        for c in range(cols):
            out[:, c * LANES : (c + 1) * LANES] = acc[c]

    smem = pl.BlockSpec(memory_space=pltpu.SMEM)
    vmem = pl.BlockSpec(memory_space=pltpu.VMEM)
    return pl.pallas_call(
        kernel,
        out_shape=jax.ShapeDtypeStruct((rows, width), jnp.float32),
        in_specs=[smem, smem, vmem, vmem],
        out_specs=vmem,
        scratch_shapes=[pltpu.VMEM((cols, rows, LANES), jnp.float32)],
        cost_estimate=pl.CostEstimate(flops=10**7, bytes_accessed=10**6, transcendentals=0),
        name="keep",
    )(cnt, sel, grad, res)


def merge_call(parts, slots, own_blocks, chunk):
    per = LANES // slots

    def kernel(*refs):
        out = refs[-1]
        views = []
        for ref in refs[:-1]:
            views += [ref] if len(ref.shape) == 2 else [ref.at[i] for i in range(ref.shape[0])]
        block = lax.broadcasted_iota(jnp.int32, (own_blocks, LANES), 0).astype(jnp.float32)
        total = jnp.zeros((own_blocks, LANES), jnp.float32)
        for at in range(0, len(views), chunk):
            group = views[at : at + chunk]
            ids = group[0][slots : slots + 1, :]
            for view in group[1:]:
                ids = jnp.maximum(ids, view[slots : slots + 1, :])
            x = [view[:slots, :] for view in group]
            x += [jnp.zeros((slots, LANES), jnp.float32)] * (per - len(group))
            x = jnp.concatenate(x, axis=0)
            hot = (block == ids).astype(jnp.float32).astype(jnp.bfloat16)
            high = x.astype(jnp.bfloat16)
            left = x - high.astype(jnp.float32)
            mid = left.astype(jnp.bfloat16)
            low = (left - mid.astype(jnp.float32)).astype(jnp.bfloat16)
            for piece in (high, mid, low):
                total = total + jnp.dot(hot, piece, preferred_element_type=jnp.float32)
        out[...] = total

    vmem = pl.BlockSpec(memory_space=pltpu.VMEM)
    return pl.pallas_call(
        kernel,
        out_shape=pltpu.VMEM((own_blocks, LANES), jnp.float32),
        in_specs=[vmem] * len(parts),
        out_specs=vmem,
        name="merge",
    )(*[pltpu.with_memory_space_constraint(p, pltpu.VMEM) for p in parts])


def xor_send(x, axis, size, k):
    return lax.ppermute(x, axis, [(i, i ^ k) for i in range(size)])


def group_sum(x, groups, bit):
    if not is_pow2(groups):
        return jnp.sum(lax.all_gather(x, "grp"), axis=0)
    while bit < groups:
        wide = bit > 1 and bit * 2 < groups
        hops = (bit, 2 * bit, 3 * bit) if wide else (bit,)
        x = sum([xor_send(x, "grp", groups, k) for k in hops], x)
        bit *= 4 if wide else 2
    return x


def make_body(groups, shards):
    by_xor = is_pow2(shards) and shards <= 8
    early = by_xor and is_pow2(groups) and groups > 1

    def body(gradient, residual, selected, counts):
        rows, width = gradient.shape[2:]
        own_rows = rows // shards
        own_blocks = own_rows * width // LANES
        slots = selected.shape[3]
        grad, res, sel, cnt = gradient[0, 0], residual[0, 0], selected[0, 0], counts[0, 0]
        info = lax.axis_index("wide").astype(jnp.int32).reshape(1)
        packed = pick_call(grad, res, sel, cnt, info, shards, own_rows, by_xor)
        if by_xor:
            parts = [xor_send(packed[k], "wide", shards, k) for k in reversed(range(1, shards))]
            parts = [packed[0]] + parts[::-1]
            if early:
                parts += [xor_send(part, "grp", groups, 1) for part in parts]
        else:
            parts = [lax.all_to_all(packed[0], "wide", split_axis=0, concat_axis=0, tiled=True)]
        new_residual = keep_call(grad, res, sel, cnt, own_rows)[None, None]
        chunk = min(LANES // slots, shards)
        partial = merge_call(parts, slots, own_blocks, chunk)
        total = group_sum(partial, groups, 2 if early else 1) / groups
        update = total.reshape(width // LANES, own_rows, LANES).transpose(1, 0, 2)
        return (update.reshape(1, own_rows, width), new_residual)

    return body


def solution(mesh):
    return jax.shard_map(
        make_body(mesh.shape["grp"], mesh.shape["wide"]),
        mesh=mesh,
        in_specs=(
            P("grp", "wide", None, None),
            P("grp", "wide", None, None),
            P("grp", "wide", None, None),
            P("grp", "wide", None),
        ),
        out_specs=(P("wide", None, None), P("grp", "wide", None, None)),
        check_vma=False,
    )
```
